32 devices in a mesh: groups: 2 (over x), section: 16 (over z, y, core).
Axes of the slice: x: 2, y: 2, z: 4, core: 2. Of those that a mesh axis runs over, the one named last changes fastest.
Arguments:
- tiles: float32 [32, 256, 256], P(('groups', 'section')), parts along dimension 0, may hold values from -6 to 6
- partners: int32 [32, 3], P(('groups', 'section')), parts along dimension 0, may hold values from 0 to 1, as said below
Outputs:
- shifts: float32 [32, 3, 9, 1024], P(('groups', 'section')), parts along dimension 0
The draws below stay inside these ranges and needn't reach their ends.
There are 2 independent parts, one for each index of `groups`. The reference program is written for one: setup_inputs(seed, part) draws one part's arguments, and reference() takes and returns one part's arrays. A program takes and returns all parts, laid end to end along the dimension named above; each array names one. Nothing has to cross between parts.
Inputs may be any that keep to these rules, and one draw needn't show every extreme that they name: `partners`: every section lists at least one partner offset.
All inputs are finite; a program needn't handle non-finite values.
Results may differ from the reference program's by a relative error of at most 0.00007.
Values sent between devices are 32-bit elements; how exact they have to be, the bound alone decides.
No kernel may reach another device: no remote copies, remote signals or barrier semaphores. Data moves between devices by JAX's collectives and lax.ppermute only.
A program may use at most 64 MiB of HBM per device.

```python
import jax
import jax.numpy as jnp
from jax import lax

PATCH = 128
TILE = 128
REACH = 3
CROP = 32
GRID = 3
SECTIONS = 16


def draw_partners(key, part):
    random_bits = jax.random.randint(jax.random.fold_in(key, 11), (SECTIONS, REACH), 0, 2)
    chosen = jax.random.randint(jax.random.fold_in(key, 12), (SECTIONS, 1), 0, REACH)
    forced = (jnp.arange(REACH, dtype=jnp.int32)[None, :] == chosen).astype(jnp.int32)
    return jnp.maximum(random_bits, forced).astype(jnp.int32)


def shard_levels(own_key, extent, pieces, least, high):
    factor_of = 1.0
    for axis_at, blocks in pieces:
        draws = jax.random.uniform(jax.random.fold_in(jax.random.fold_in(own_key, 6), axis_at), (blocks,), jnp.float32, least / len(pieces), high / len(pieces))
        factor_of = factor_of * jnp.repeat(jnp.exp(draws), extent[axis_at] // blocks).reshape((-1,) + (1,) * (len(extent) - 1 - axis_at))
    return factor_of


def gaussian(stream_key, extent, width, most, pieces=(), held_as=jnp.bfloat16):
    drawn = jax.random.normal(stream_key, extent, jnp.float32) * width
    if len(pieces) > 0:
        drawn = shard_levels(stream_key, extent, pieces, -0.22, 0.18) * drawn
    return jnp.clip(drawn, min=-most, max=most).astype(held_as)


def setup_inputs(seed: int = 0, part: int = 0) -> dict:
    key_list = jax.random.split(jax.random.key(seed), 3)
    own_keys = jax.random.split(jax.random.fold_in(key_list[2], part), 3)
    tiles = gaussian(own_keys[0], (SECTIONS, TILE + PATCH, TILE + PATCH), 1.0, 6.0, ((0, 16),), jnp.float32)
    partners = draw_partners(jax.random.fold_in(jax.random.fold_in(key_list[2], part), 71), part)
    return {"tiles": tiles, "partners": partners}


def cut_patches(tiles, patch):
    count = tiles.shape[0]
    stride = patch // 2
    grid = tiles.shape[-1] // stride - 1
    blocks = tiles.reshape(count, grid + 1, stride, grid + 1, stride)
    rowwise = jnp.concatenate([blocks[:, :-1], blocks[:, 1:]], axis=2)
    joined = jnp.concatenate([rowwise[:, :, :, :-1], rowwise[:, :, :, 1:]], axis=4)
    return joined.transpose(0, 1, 3, 2, 4).reshape(count, grid * grid, patch, patch)

def standardize(patches):
    middle = lax.optimization_barrier(jnp.mean(patches, axis=(-2, -1), keepdims=True))
    centred = patches - middle
    spread = jnp.sqrt(lax.optimization_barrier(jnp.mean(centred * centred, axis=(-2, -1), keepdims=True)) + 1e-06)
    return centred / spread

def reference(tiles, partners):
    kept = jnp.concatenate([jnp.arange(PATCH - CROP // 2, PATCH), jnp.arange(0, CROP // 2)]).astype(jnp.int32)

    def spectrum(tile):
        return jnp.fft.fft2(standardize(cut_patches(tile[None], PATCH))[0])
    spectra = lax.map(spectrum, tiles)
    padded = jnp.concatenate([spectra, jnp.zeros((REACH,) + spectra.shape[1:], spectra.dtype)], axis=0)

    def one_section(index):
        mine = spectra[index]
        others = lax.dynamic_slice_in_dim(padded, index + 1, REACH, 0)
        whole = jnp.real(jnp.fft.ifft2(jnp.conj(mine)[None] * others))
        block = jnp.take(jnp.take(whole, kept, axis=2), kept, axis=3)
        return (block / PATCH).reshape(REACH, GRID * GRID, CROP * CROP)
    result = lax.map(one_section, jnp.arange(SECTIONS, dtype=jnp.int32))
    where_sec = jnp.arange(SECTIONS, dtype=jnp.int32)[:, None]
    offsets = jnp.arange(REACH, dtype=jnp.int32)[None, :] + 1
    listed = (partners == 1) & (where_sec + offsets < SECTIONS)
    return jnp.where(listed[:, :, None, None], result, 0.0).astype(jnp.float32)
```

```python
import functools
import math

import jax
import jax.numpy as jnp
import numpy as np
from jax import lax
from jax.experimental import pallas as pl
from jax.experimental.pallas import tpu as pltpu
from jax.sharding import PartitionSpec as P

PATCH = 128
REACH = 3
CROP = 32
GRID = 3
HALF = PATCH // 2
SIDE = PATCH + HALF * (GRID - 1)
LANES = 512
ROWS = 144


def halves(table):
    top = table.astype(jnp.bfloat16)
    return top, (table - top.astype(np.float32)).astype(jnp.bfloat16)


def tables():
    y = np.arange(SIDE)
    freq = np.arange(HALF)
    first = np.zeros((SIDE, LANES))
    back = np.zeros((LANES, 128))
    shift = np.arange(CROP) - CROP // 2
    weight = np.where(freq == 0, 1.0, 2.0)
    for j in range(GRID):
        inside = ((y >= HALF * j) & (y < HALF * j + PATCH))[:, None]
        angle = 2 * math.pi * ((y[:, None] - HALF * j) * freq[None, :] % PATCH) / PATCH
        col = 256 * (j // 2) + HALF * (j % 2)
        first[:, col : col + HALF] = np.where(inside, np.cos(angle), 0)
        first[:, col + 128 : col + 128 + HALF] = np.where(inside, np.sin(angle), 0)
        ny = 256 + HALF + j
        first[:, ny] = np.where(inside[:, 0], 1.0 - 2.0 * (y % 2), 0)
        angle = 2 * math.pi * (freq[:, None] * shift[None, :] % PATCH) / PATCH
        out = slice(CROP * j, CROP * j + CROP)
        back[col : col + HALF, out] = weight[:, None] * np.cos(angle)
        back[col + 128 : col + 128 + HALF, out] = weight[:, None] * np.sin(angle)
        back[ny, out] = 1.0 - 2.0 * (shift % 2)
    x = np.arange(PATCH)
    angle = 2 * math.pi * (freq[:, None] * x[None, :] % PATCH) / PATCH
    second = np.zeros((ROWS, PATCH))
    second[:HALF] = np.cos(angle)
    second[HALF:PATCH] = np.sin(angle)
    second[PATCH] = 1.0 - 2.0 * (x % 2)
    angle = 2 * math.pi * (freq[None, :] * shift[:, None] % PATCH) / PATCH
    last = np.zeros((CROP, ROWS))
    last[:, :HALF] = weight * np.cos(angle)
    last[:, HALF:PATCH] = weight * np.sin(angle)
    last[:, PATCH] = 1.0 - 2.0 * (shift % 2)
    pick = np.zeros((SIDE, 128), np.float32)
    for j in range(GRID):
        pick[HALF * j : HALF * j + PATCH, CROP * j : CROP * j + CROP] = 1.0
    f_h, f_l = halves(first.astype(np.float32))
    s_h, s_l = halves(second.astype(np.float32))
    b_h, b_l = halves(back.astype(np.float32))
    l_h, l_l = halves(last.astype(np.float32))
    return (
        f_h,
        f_l,
        np.concatenate([s_h, s_h], axis=1),
        s_l,
        np.concatenate([b_h, b_l], axis=1),
        np.concatenate([l_h, l_l], axis=0),
        pick.astype(jnp.bfloat16),
    )


def mul(a, b):
    return jnp.dot(a, b, preferred_element_type=jnp.float32)


def split(x):
    top = x.astype(jnp.bfloat16)
    return top, (x - top.astype(jnp.float32)).astype(jnp.bfloat16)


def rows_of(tile, f_h, f_l):
    tile = tile - jnp.mean(tile)
    top, low = split(tile)
    segment = mul(top, f_h) + mul(low, f_h) + mul(top, f_l)
    return tile, split(segment)


def spread_of(tile, pick):
    square = tile * tile
    sums = []
    for values in (tile, square):
        for i in range(GRID):
            sums.append(jnp.sum(values[HALF * i : HALF * i + PATCH], axis=0, keepdims=True))
    sums.append(jnp.zeros((16 - len(sums), SIDE), jnp.float32))
    top, low = split(jnp.concatenate(sums, axis=0))
    means = (mul(top, pick) + mul(low, pick)) * (1.0 / PATCH**2)
    return [lax.rsqrt(means[GRID + i : GRID + i + 1] - means[i : i + 1] ** 2 + 1e-06) for i in range(GRID)]


def columns_of(segment, i, s_hh, s_l):
    top, low = (part[HALF * i : HALF * i + PATCH] for part in segment)
    return mul(s_hh, jnp.concatenate([top, low], axis=0)) + mul(s_l, top)


def power(a, b, sign):
    out = []
    for g in range(2):
        acc, acs, asc, ass = a(0, 2 * g), a(0, 2 * g + 1), a(1, 2 * g), a(1, 2 * g + 1)
        bcc, bcs, bsc, bss = b(0, 2 * g), b(0, 2 * g + 1), b(1, 2 * g), b(1, 2 * g + 1)
        anc, ans, bnc, bns = a(2, 2 * g), a(2, 2 * g + 1), b(2, 2 * g), b(2, 2 * g + 1)
        cc = (acc * bcc + asc * bsc) + (acs * bcs + ass * bss)
        ss = (acc * bss + ass * bcc) - (acs * bsc + asc * bcs)
        sc = (acs * bss - ass * bcs) + (acc * bsc - asc * bcc)
        cs = (acc * bcs - acs * bcc) + (asc * bss - ass * bsc)
        nc = anc * bnc + ans * bns
        ns = anc * bns - ans * bnc
        if sign < 0:
            sc, cs, ns = -sc, -cs, -ns
        zero = jnp.zeros_like(nc)
        out.append(jnp.concatenate([cc, sc, nc, zero], axis=0))
        out.append(jnp.concatenate([cs, ss, ns, zero], axis=0))
    return jnp.concatenate(out, axis=1)


def shifts_of(product, b_hl, l_hl):
    top, low = split(product)
    wide = mul(top, b_hl)
    half = wide[:, :128] + wide[:, 128:] + mul(low, b_hl[:, :128])
    top, low = split(half)
    wide = mul(l_hl, jnp.concatenate([top, low], axis=1))
    return wide[:CROP, :128] + wide[:CROP, 128:] + wide[CROP:, :128]


BANDS = ((0, HALF), (HALF, PATCH), (PATCH, PATCH + 8))


def own_kernel(tile, f_h, f_l, s_hh, s_l, pick, spec, spread):
    values, segment = rows_of(tile[...], f_h[...], f_l[...])
    lane = lax.broadcasted_iota(jnp.int32, (8, LANES), 1)
    row = lax.broadcasted_iota(jnp.int32, (8, LANES), 0)
    constant = (row == 0) & ((lane == 0) | (lane == HALF) | (lane == 256))
    for i in range(GRID):
        part = columns_of(segment, i, s_hh[...], s_l[...])
        spec[i] = part
        spec[i, 0:8, :] = jnp.where(constant, 0.0, part[0:8])
    for i, value in enumerate(spread_of(values, pick[...])):
        spread[i : i + 1, :] = value


def pair_kernel(sign, tile, spec, spread, f_h, f_l, s_hh, s_l, b_hl, l_hl, pick, out):
    values, segment = rows_of(tile[...], f_h[...], f_l[...])
    other = spread_of(values, pick[...])
    for i in range(GRID):
        part = columns_of(segment, i, s_hh[...], s_l[...])
        own = lambda r, c, i=i: spec[i, BANDS[r][0] : BANDS[r][1], 128 * c : 128 * c + 128]
        new = lambda r, c, part=part: part[BANDS[r][0] : BANDS[r][1], 128 * c : 128 * c + 128]
        result = shifts_of(power(own, new, sign), b_hl[...], l_hl[...])
        scale = spread[i : i + 1, :] * other[i] * (1.0 / float(PATCH**3))
        out[i] = result * scale


def call(kernel, outs, *args):
    vmem = pl.BlockSpec(memory_space=pltpu.VMEM)
    return pl.pallas_call(
        kernel,
        out_shape=outs,
        in_specs=[vmem] * len(args),
        out_specs=jax.tree.map(lambda _: vmem, outs),
        cost_estimate=pl.CostEstimate(flops=4_000_000_000, bytes_accessed=2_000_000, transcendentals=0),
    )(*args)


def body(tiles, partners):
    f_h, f_l, s_hh, s_l, b_hl, l_hl, pick = (jnp.asarray(t) for t in tables())
    total = lax.axis_size("section")
    position = lax.axis_index("section")
    even = position % 2 == 0
    send = functools.partial(lax.ppermute, axis_name="section")
    ahead = [(i, i + (1 if i % 2 == 0 else 3)) for i in range(total)]
    ahead = [(i, j) for i, j in ahead if j < total]
    swap = [(i, i ^ 1) for i in range(total)]
    direct = send(tiles, perm=[(i, i - 2) for i in range(2, total)])
    early = send(tiles, perm=ahead)
    relay = send(direct, perm=swap)
    spec, spread = call(
        own_kernel,
        (jax.ShapeDtypeStruct((GRID, ROWS, LANES), jnp.float32), jax.ShapeDtypeStruct((8, 128), jnp.float32)),
        tiles[0], f_h, f_l, s_hh, s_l, pick,
    )
    block = jax.ShapeDtypeStruct((GRID, CROP, 128), jnp.float32)

    def pair(tile, sign):
        return call(functools.partial(pair_kernel, sign), block, tile[0], spec, spread, f_h, f_l, s_hh, s_l, b_hl, l_hl, pick)

    back = send(pair(early, -1), perm=[(j, i) for i, j in ahead])
    second = pair(direct, 1)
    third = pair(relay, 1)
    result = jnp.stack([jnp.where(even, back, third), second, jnp.where(even, third, back)])
    result = result[..., : GRID * CROP].reshape(REACH, GRID, CROP, GRID, CROP).transpose(0, 1, 3, 2, 4)
    result = result.reshape(REACH, GRID * GRID, CROP * CROP)
    offsets = jnp.arange(REACH, dtype=jnp.int32) + 1
    listed = (partners[0] == 1) & (position + offsets < total)
    return jnp.where(listed[:, None, None], result, 0.0)[None]


def solution(mesh):
    in_specs = (P(("groups", "section"), None, None), P(("groups", "section"), None))
    out_specs = P(("groups", "section"), None, None, None)
    return jax.shard_map(body, mesh=mesh, in_specs=in_specs, out_specs=out_specs, check_vma=False)
```

```python
import functools
import math

import jax
import jax.numpy as jnp
import numpy as np
from jax import lax
from jax.experimental import pallas as pl
from jax.experimental.pallas import tpu as pltpu
from jax.sharding import PartitionSpec as P


PATCH = 128
REACH = 3
CROP = 32
GRID = 3
HALF = PATCH // 2
SIDE = PATCH + HALF * (GRID - 1)
LANES = 512
ROWS = 144


PLACES = {
    "first_h": (slice(0, SIDE), slice(0, LANES)),
    "first_l": (slice(SIDE, 2 * SIDE), slice(0, LANES)),
    "back": (slice(512, 1024), slice(0, 256)),
    "second": (slice(512, 656), slice(256, 512)),
    "second_l": (slice(656, 800), slice(256, 384)),
    "last": (slice(912, 976), slice(256, 400)),
    "pick": (slice(656, 912), slice(384, 512)),
}


def halves(table):
    top = table.astype(jnp.bfloat16)
    return top, (table - top.astype(np.float32)).astype(jnp.bfloat16)


def tables():
    y = np.arange(SIDE)
    freq = np.arange(HALF)
    first = np.zeros((SIDE, LANES))
    back = np.zeros((LANES, 128))
    shift = np.arange(CROP) - CROP // 2
    weight = np.where(freq == 0, 1.0, 2.0)
    for j in range(GRID):
        inside = ((y >= HALF * j) & (y < HALF * j + PATCH))[:, None]
        angle = 2 * math.pi * ((y[:, None] - HALF * j) * freq[None, :] % PATCH) / PATCH
        col = 256 * (j // 2) + HALF * (j % 2)
        first[:, col : col + HALF] = np.where(inside, np.cos(angle), 0)
        first[:, col + 128 : col + 128 + HALF] = np.where(inside, np.sin(angle), 0)
        ny = 256 + HALF + j
        first[:, ny] = np.where(inside[:, 0], 1.0 - 2.0 * (y % 2), 0)
        angle = 2 * math.pi * (freq[:, None] * shift[None, :] % PATCH) / PATCH
        out = slice(CROP * j, CROP * j + CROP)
        back[col : col + HALF, out] = weight[:, None] * np.cos(angle)
        back[col + 128 : col + 128 + HALF, out] = weight[:, None] * np.sin(angle)
        back[ny, out] = 1.0 - 2.0 * (shift % 2)
    x = np.arange(PATCH)
    angle = 2 * math.pi * (freq[:, None] * x[None, :] % PATCH) / PATCH
    second = np.zeros((ROWS, PATCH))
    second[:HALF] = np.cos(angle)
    second[HALF:PATCH] = np.sin(angle)
    second[PATCH] = 1.0 - 2.0 * (x % 2)
    angle = 2 * math.pi * (freq[None, :] * shift[:, None] % PATCH) / PATCH
    last = np.zeros((CROP, ROWS))
    last[:, :HALF] = weight * np.cos(angle)
    last[:, HALF:PATCH] = weight * np.sin(angle)
    last[:, PATCH] = 1.0 - 2.0 * (shift % 2)
    pick = np.zeros((SIDE, 128), np.float32)
    for j in range(GRID):
        pick[HALF * j : HALF * j + PATCH, CROP * j : CROP * j + CROP] = 1.0
    packed = np.zeros((1024, LANES), np.float32)
    f_h, f_l = halves(first.astype(np.float32))
    s_h, s_l = halves(second.astype(np.float32))
    b_h, b_l = halves(back.astype(np.float32))
    l_h, l_l = halves(last[[4 * q + r for r in range(4) for q in range(CROP // 4)]].astype(np.float32))
    for (rows, cols), table in zip(
        PLACES.values(),
        (
            f_h,
            f_l,
            np.concatenate([b_h, b_l], axis=1),
            np.concatenate([s_h, s_h], axis=1),
            s_l,
            np.concatenate([l_h, l_l], axis=0),
            pick,
        ),
        strict=True,
    ):
        packed[rows, cols] = table
    return packed.astype(jnp.bfloat16)


def mul(a, b):
    return jnp.dot(a, b, preferred_element_type=jnp.float32)


def split(x):
    top = x.astype(jnp.bfloat16)
    return top, (x - top.astype(jnp.float32)).astype(jnp.bfloat16)


def rows_of(tile, table):
    tile = tile - jnp.mean(tile)
    top, low = split(tile)
    first = table("first_h")
    return tile, split(mul(top, first) + mul(low, first) + mul(top, table("first_l")))


def spread_of(tile, table):
    square = tile * tile
    sums = []
    for values in (tile, square):
        for i in range(GRID):
            sums.append(jnp.sum(values[HALF * i : HALF * i + PATCH], axis=0, keepdims=True))
    sums.append(jnp.zeros((16 - len(sums), SIDE), jnp.float32))
    top, low = split(jnp.concatenate(sums, axis=0))
    means = (mul(top, table("pick")) + mul(low, table("pick"))) * (1.0 / PATCH**2)
    return [lax.rsqrt(means[GRID + i : GRID + i + 1] - means[i : i + 1] ** 2 + 1e-06) for i in range(GRID)]


def columns_of(segment, i, table):
    top, low = (part[HALF * i : HALF * i + PATCH] for part in segment)
    return mul(table("second"), jnp.concatenate([top, low], axis=0)) + mul(table("second_l"), top)


def power(a, b):
    out = []
    for g in range(2):
        acc, acs, asc, ass = a(0, 2 * g), a(0, 2 * g + 1), a(1, 2 * g), a(1, 2 * g + 1)
        bcc, bcs, bsc, bss = b(0, 2 * g), b(0, 2 * g + 1), b(1, 2 * g), b(1, 2 * g + 1)
        anc, ans, bnc, bns = a(2, 2 * g), a(2, 2 * g + 1), b(2, 2 * g), b(2, 2 * g + 1)
        cc = (acc * bcc + asc * bsc) + (acs * bcs + ass * bss)
        ss = (acc * bss + ass * bcc) - (acs * bsc + asc * bcs)
        sc = (acs * bss - ass * bcs) + (acc * bsc - asc * bcc)
        cs = (acc * bcs - acs * bcc) + (asc * bss - ass * bsc)
        nc = anc * bnc + ans * bns
        ns = anc * bns - ans * bnc
        zero = jnp.zeros_like(nc)
        out.append(jnp.concatenate([cc, sc, nc, zero], axis=0))
        out.append(jnp.concatenate([cs, ss, ns, zero], axis=0))
    return jnp.concatenate(out, axis=1)


def shifts_of(products, table):
    parts = [split(product) for product in products]
    count = len(parts)
    wide = mul(jnp.concatenate([top for top, _ in parts] + [low for _, low in parts], axis=0), table("back"))
    out = []
    for i in range(count):
        top, low = (wide[ROWS * k : ROWS * k + ROWS] for k in (i, count + i))
        top, low = split((top[:, :128] + top[:, 128:]) + (low[:, :128] + low[:, 128:]))
        ends = mul(table("last"), jnp.concatenate([top, low], axis=1))
        out.append(ends[:CROP, :128] + ends[:CROP, 128:] + (ends[CROP:, :128] + ends[CROP:, 128:]))
    return out


def patches_of(block):
    lane = lax.broadcasted_iota(jnp.int32, (8, 128), 1) // CROP
    rows = [block[8 * r : 8 * r + 8] for r in range(4)]
    out = []
    for j in range(GRID):
        moved = [rows[r] if r == j else pltpu.roll(rows[r], CROP * ((r - j) % 4), 1) for r in range(4)]
        out.append(jnp.where(lane < 2, jnp.where(lane == 0, moved[0], moved[1]), jnp.where(lane == 2, moved[2], moved[3])))
    return out


BANDS = ((0, HALF), (HALF, PATCH), (PATCH, PATCH + 8))


def reader(packed):
    return lambda name: packed[PLACES[name][0], PLACES[name][1]]


def own_kernel(tile, packed, spec, spread):
    table = reader(packed)
    values, segment = rows_of(tile[...], table)
    lane = lax.broadcasted_iota(jnp.int32, (8, LANES), 1)
    row = lax.broadcasted_iota(jnp.int32, (8, LANES), 0)
    constant = (row == 0) & ((lane == 0) | (lane == HALF) | (lane == 256))
    for i in range(GRID):
        part = columns_of(segment, i, table)
        spec[i] = part
        spec[i, 0:8, :] = jnp.where(constant, 0.0, part[0:8])
    for i, value in enumerate(spread_of(values, table)):
        spread[i : i + 1, :] = value


def pair(tile, spec, spread, packed):
    table = reader(packed)
    values, segment = rows_of(tile[...], table)
    other = spread_of(values, table)
    products = []
    for i in range(GRID):
        part = columns_of(segment, i, table)
        own = lambda r, c, i=i: spec[i, BANDS[r][0] : BANDS[r][1], 128 * c : 128 * c + 128]
        new = lambda r, c, part=part: part[BANDS[r][0] : BANDS[r][1], 128 * c : 128 * c + 128]
        products.append(power(own, new))
    out = []
    for i, block in enumerate(shifts_of(products, table)):
        out += patches_of(block * (spread[i : i + 1, :] * other[i] * (1.0 / float(PATCH**3))))
    return out


def pair_kernel(tile, spec, spread, packed, out):
    for p, block in enumerate(pair(tile, spec, spread, packed)):
        out[8 * p : 8 * p + 8, :] = block


def final_kernel(partners, tile, spec, spread, packed, second, third, out, turned):
    position = lax.axis_index("section")
    total = lax.axis_size("section")
    even = position % 2 == 0

    def place(slot, p, value):
        turned[slot, pl.ds(p, 8, stride=16), :] = value

    listed = [(partners[0, slot] == 1) & (position + (slot + 1) < total) for slot in range(REACH)]
    for p in range(GRID * GRID):
        place(1, p, jnp.where(listed[1], second[8 * p : 8 * p + 8, :], 0.0))
    for p, value in enumerate(pair(tile, spec, spread, packed)):
        passed = third[8 * p : 8 * p + 8, :]
        place(0, p, jnp.where(listed[0], jnp.where(even, value, passed), 0.0))
        place(2, p, jnp.where(listed[2], jnp.where(even, passed, value), 0.0))
    for slot in range(REACH):
        for q in range(8):
            out[0, slot, 0:8, 128 * q : 128 * q + 128] = turned[slot, 16 * q : 16 * q + 8, :]
            out[0, slot, 8:9, 128 * q : 128 * q + 128] = turned[slot, 16 * q + 8 : 16 * q + 9, :]


def call(kernel, outs, *args, scalars=0, scratch=()):
    vmem = pl.BlockSpec(memory_space=pltpu.VMEM)
    smem = pl.BlockSpec(memory_space=pltpu.SMEM)
    return pl.pallas_call(
        kernel,
        out_shape=outs,
        in_specs=[smem] * scalars + [vmem] * (len(args) - scalars),
        out_specs=jax.tree.map(lambda _: vmem, outs),
        scratch_shapes=scratch,
        compiler_params=pltpu.CompilerParams(vmem_limit_bytes=16 * 1024 * 1024),
        cost_estimate=pl.CostEstimate(flops=4_000_000_000, bytes_accessed=2_000_000, transcendentals=0),
    )(*args)


def body(tiles, partners):
    packed = jnp.asarray(tables())
    total = lax.axis_size("section")
    send = functools.partial(lax.ppermute, axis_name="section")
    near = [(i, i - (1 if i % 2 else 3)) for i in range(total)]
    near = [(i, j) for i, j in near if j >= 0]
    spectra = (jax.ShapeDtypeStruct((GRID, ROWS, LANES), jnp.float32), jax.ShapeDtypeStruct((8, 128), jnp.float32))
    block = jax.ShapeDtypeStruct((8 * GRID * GRID, 128), jnp.float32)
    direct = send(tiles, perm=[(i, i - 2) for i in range(2, total)])
    early = send(tiles, perm=near)
    relay = send(direct, perm=[(i, i ^ 1) for i in range(total)])
    spec, spread = call(own_kernel, spectra, tiles[0], packed)
    second = call(pair_kernel, block, direct[0], spec, spread, packed)
    third = call(pair_kernel, block, relay[0], spec, spread, packed)
    return call(
        final_kernel,
        jax.ShapeDtypeStruct((1, REACH, GRID * GRID, CROP * CROP), jnp.float32),
        partners, early[0], spec, spread, packed, second, third,
        scalars=1,
        scratch=[pltpu.VMEM((REACH, 128, 128), jnp.float32)],
    )


def solution(mesh):
    in_specs = (P(("groups", "section"), None, None), P(("groups", "section"), None))
    out_specs = P(("groups", "section"), None, None, None)
    return jax.shard_map(body, mesh=mesh, in_specs=in_specs, out_specs=out_specs, check_vma=False)
```
